32 devices in a mesh: lat: 4 (over z), lon: 8 (over y, x, core).
Axes of the slice: x: 2, y: 2, z: 4, core: 2. Of those that a mesh axis runs over, the one named last changes fastest.
Arguments:
- surface_forcing: float32 [4320, 1024], P('lon', 'lat'), may hold values from -40 to 40
- ocean_mask: int32 [4320, 1024], P('lon', 'lat'), may hold values 0 or 1
- self_coupling: float32 [4320, 1024], P('lon', 'lat'), may hold values from 0.2 to 2
- east_coupling: float32 [4320, 1024], P('lon', 'lat'), may hold values from 0.3 to 3
- north_coupling: float32 [4320, 1024], P('lon', 'lat'), may hold values from 0.3 to 3
- zonal_weight: float32 [1024], P('lat'), may hold values from 0.5 to 50
- aligned_inverse: float32 [8, 128, 128], P('lat'), may hold values from -1 to 4, as said below
- staggered_inverse: float32 [8, 128, 128], P('lat'), may hold values from -1 to 4, as said below
Outputs:
- solution: float32 [4320, 1024], P('lon', 'lat')
- residual: float32 [4320, 1024], P('lon', 'lat')
- direction: float32 [4320, 1024], P('lon', 'lat')
The draws below stay inside these ranges and needn't reach their ends.
Inputs may be any that keep to these rules, and one draw needn't show every extreme that they name: `aligned_inverse`: each block is symmetric and positive definite. `staggered_inverse`: each block is symmetric and positive definite.
All inputs are finite; a program needn't handle non-finite values. No bound on the sum of `ocean_mask` on one device may be relied on, other than what follows from the above.
Results may differ from the reference program's by a relative error of at most 0.00023.
Values sent between devices are 32-bit elements; how exact they have to be, the bound alone decides.
A program may use at most 64 MiB of HBM per device.

```python
import math
import jax
import jax.numpy as jnp
from jax import lax

NLON = 4320
BL = 128
NLAT = 1024
NBLK = 8


def draw_surface_forcing(key, part):
    first = jax.random.fold_in(jax.random.fold_in(key, 7), 0)
    lon_pos = jnp.arange(NLON).astype(jnp.float32) / NLON
    lat_pos = jnp.arange(NLAT).astype(jnp.float32) / NLAT
    ramp = (1.0 + 2.0 * lon_pos)[:, None] * (1.0 + 2.0 * lat_pos)[None, :]
    values = ramp * jnp.clip(jax.random.normal(first, (NLON, NLAT), jnp.float32), -4.4, 4.4)
    return values


def inverse_blocks(key, ratio, lowest, highest):
    first, second = jax.random.split(key, 2)
    index = jnp.arange(BL)
    distance = jnp.abs(index[:, None] - index[None, :]).astype(jnp.float32)
    decaying = jnp.power(jnp.float32(ratio), distance)
    mixing = jax.random.uniform(first, (NBLK, BL, BL), jnp.float32, -1.0, 1.0)
    gram = jnp.einsum('bij,bkj->bik', mixing, mixing) / (2.0 * BL)
    core = 0.5 * jnp.eye(BL, dtype=jnp.float32)[None] + decaying[None] + gram
    scales = jnp.exp(jax.random.uniform(second, (NBLK, BL), jnp.float32, jnp.log(lowest), jnp.log(highest)))
    return 0.3 * scales[:, :, None] * core * scales[:, None, :]


def draw_aligned_inverse(key, part):
    return inverse_blocks(jax.random.fold_in(key, 11), 0.6, 0.5, 2.0)


def draw_staggered_inverse(key, part):
    return inverse_blocks(jax.random.fold_in(key, 23), 0.6, 0.5, 2.0)


def place_ends(array, stream_key, smallest, high):
    extent = array.shape
    spot = [jax.random.randint(jax.random.fold_in(stream_key, axis), (), 0, extent[axis]) for axis in range(len(extent))]
    array = array.at[tuple(spot)].set(smallest)
    longest = extent.index(max(extent))
    spot[longest] = (spot[longest] + 1) % extent[longest]
    return array.at[tuple(spot)].set(high)


def shard_levels(key, extent, cuts, smallest, top_value):
    factor_of = 1.0
    for dim, shards_of in cuts:
        steps = jax.random.uniform(jax.random.fold_in(jax.random.fold_in(key, 6), dim), (shards_of,), jnp.float32, smallest / len(cuts), top_value / len(cuts))
        factor_of = factor_of * jnp.repeat(jnp.exp(steps), extent[dim] // shards_of).reshape((-1,) + (1,) * (len(extent) - 1 - dim))
    return factor_of


def setup_inputs(seed: int = 0) -> dict:
    keys = jax.random.split(jax.random.key(seed), 9)
    return {
        "surface_forcing": draw_surface_forcing(jax.random.fold_in(keys[8], 71), 0),
        "ocean_mask": place_ends((jax.random.randint(keys[1], (NLON, NLAT), 0, 5) < 4).astype(jnp.int32), jax.random.fold_in(keys[1], 1), 0, 1),
        "self_coupling": jnp.clip(jnp.exp(math.log(2.0) - 2.3025851 * jax.random.uniform(keys[2], (NLON, NLAT), jnp.float32) ** shard_levels(keys[2], (NLON, NLAT), ((0, 8), (1, 4)), -0.2, 0.2)), 0.2, 2.0),
        "east_coupling": jnp.clip(jnp.exp(math.log(3.0) - 2.3025851 * jax.random.uniform(keys[3], (NLON, NLAT), jnp.float32) ** shard_levels(keys[3], (NLON, NLAT), ((0, 8), (1, 4)), -0.2, 0.2)), 0.3, 3.0),
        "north_coupling": jnp.clip(jnp.exp(math.log(3.0) - 2.3025851 * jax.random.uniform(keys[4], (NLON, NLAT), jnp.float32) ** shard_levels(keys[4], (NLON, NLAT), ((0, 8), (1, 4)), -0.2, 0.2)), 0.3, 3.0),
        "zonal_weight": jnp.clip(jnp.exp(math.log(50.0) - 4.6051702 * jax.random.uniform(keys[5], (NLAT,), jnp.float32) ** shard_levels(keys[5], (NLAT,), ((0, 4),), -0.2, 0.2)), 0.5, 50.0),
        "aligned_inverse": draw_aligned_inverse(jax.random.fold_in(keys[8], 71), 0),
        "staggered_inverse": draw_staggered_inverse(jax.random.fold_in(keys[8], 71), 0),
    }


FULL_TURN = 6.283185307179586

def blockwise(parts, inverse):
    shaped = parts.reshape(2, NLON, NBLK, BL)
    result = jnp.einsum('bij,smbj->smbi', inverse, shaped, precision=lax.Precision.HIGHEST)
    return result.reshape(2, NLON, NLAT)

def staggered(parts, inverse):
    half = BL // 2
    zeros = jnp.zeros((2, NLON, half), parts.dtype)
    moved = jnp.concatenate([parts[:, :, half:], zeros], axis=2)
    result = blockwise(moved, inverse)
    return jnp.concatenate([zeros, result[:, :, :NLAT - half]], axis=2)

def precondition(field, wet, zonal_weight, aligned_inverse, staggered_inverse):
    spectrum = jnp.fft.fft(field, axis=0)
    modes = jnp.arange(NLON).astype(jnp.float32)
    wave = 2.0 - 2.0 * jnp.cos(FULL_TURN * modes / NLON)
    scale = lax.rsqrt(1.0 + zonal_weight[None, :] * wave[:, None])
    parts = jnp.stack([spectrum.real, spectrum.imag]) * scale
    combined = (blockwise(parts, aligned_inverse) + staggered(parts, staggered_inverse)) * scale
    back = jnp.fft.ifft(combined[0] + 1j * combined[1], axis=0).real
    return wet * back

def reference(surface_forcing, ocean_mask, self_coupling, east_coupling, north_coupling, zonal_weight, aligned_inverse, staggered_inverse):
    wet = ocean_mask.astype(jnp.float32)
    row_index = jnp.arange(NLAT)
    top_flag = jnp.where(row_index < NLAT - 1, 1.0, 0.0).astype(jnp.float32)
    east = east_coupling * wet * jnp.roll(wet, -1, axis=0)
    north = north_coupling * wet * jnp.roll(wet, -1, axis=1) * top_flag[None, :]
    west = jnp.roll(east, 1, axis=0)
    south = jnp.roll(north, 1, axis=1)

    def operate(field):
        result = (1.0 - wet) * field + wet * self_coupling * field
        result = result + east * (field - jnp.roll(field, -1, axis=0))
        result = result + west * (field - jnp.roll(field, 1, axis=0))
        result = result + north * (field - jnp.roll(field, -1, axis=1))
        result = result + south * (field - jnp.roll(field, 1, axis=1))
        return result
    rhs_wet = wet * surface_forcing
    first = precondition(rhs_wet, wet, zonal_weight, aligned_inverse, staggered_inverse)
    rz_now = jnp.sum(rhs_wet * first)
    image = operate(first)
    curvature = jnp.sum(first * image)
    alpha = rz_now / curvature
    solution = alpha * first
    residual = rhs_wet - alpha * image
    second = precondition(residual, wet, zonal_weight, aligned_inverse, staggered_inverse)
    rz_next = jnp.sum(residual * second)
    direction = second + rz_next / rz_now * first
    return (solution, residual, direction)
```

```python
import functools

import jax
import jax.numpy as jnp
import numpy as np
from jax import lax
from jax.experimental import pallas as pl
from jax.experimental.pallas import tpu as pltpu
from jax.sharding import PartitionSpec as P

MESH = pl.DeviceIdType.MESH


def outer_table(groups):
    table = np.zeros((groups, groups))
    place = np.arange(groups)
    table[0] = 1.0
    table[1] = np.where(place % 2 == 0, 1.0, -1.0)
    for mode in range(1, groups // 2):
        turn = 2.0 * np.pi * (mode * place % groups) / groups
        table[2 * mode] = np.cos(turn)
        table[2 * mode + 1] = -np.sin(turn)
    table[np.abs(table) < 1e-12] = 0.0
    return table


def inner_tables(groups, length, padded):
    total = groups * length
    pairs = groups // 2
    matrix = np.zeros((pairs, 2 * padded, 2 * padded))
    waves = np.zeros((pairs, 2 * padded))
    weights = np.zeros((pairs, 2 * padded))
    cell = np.arange(length)

    def turns(modes):
        return 2.0 * np.pi * (modes[:, None] * cell[None, :] % total) / total

    def note(pair, start, modes):
        stop = start + len(modes)
        waves[pair, start:stop] = 2.0 - 2.0 * np.cos(2.0 * np.pi * modes / total)
        weights[pair, start:stop] = np.where(modes * 2 % total == 0, 1.0, 2.0) / total

    for part, (first, real_count) in enumerate(((0, length // 2 + 1), (groups // 2, (length + 1) // 2))):
        skipped = 1 if part == 0 else 0
        real = first + groups * np.arange(real_count)
        imag = first + groups * (skipped + np.arange(length - real_count))
        row = part * padded
        columns = slice(part * padded, part * padded + length)
        matrix[0, row : row + real_count, columns] = np.cos(turns(real))
        matrix[0, row + real_count : row + length, columns] = -np.sin(turns(imag))
        note(0, row, real)
        note(0, row + real_count, imag)
    for pair in range(1, pairs):
        modes = pair + groups * np.arange(length)
        angle = turns(modes)
        low, high = slice(0, length), slice(padded, padded + length)
        matrix[pair, low, low] = np.cos(angle)
        matrix[pair, low, high] = np.sin(angle)
        matrix[pair, high, low] = -np.sin(angle)
        matrix[pair, high, high] = np.cos(angle)
        note(pair, 0, modes)
        note(pair, padded, modes)
    single = matrix.astype(np.float32)
    leading = single.astype(jnp.bfloat16)
    rest = (matrix - leading.astype(np.float64)).astype(jnp.bfloat16)
    return np.stack([leading, rest], axis=1), waves.astype(np.float32), weights.astype(np.float32)


def parted(value):
    leading = value.astype(jnp.bfloat16)
    return leading, (value - leading.astype(jnp.float32)).astype(jnp.bfloat16)


def product(left, right):
    dot = functools.partial(jnp.dot, preferred_element_type=jnp.float32)
    return dot(left[0], right[0]) + (dot(left[0], right[1]) + dot(left[1], right[0]))


def weighted(values, factors):
    total = None
    for value, factor in zip(values, factors):
        if factor == 0.0:
            continue
        term = value if factor == 1.0 else value * np.float32(factor)
        total = term if total is None else total + term
    return total


def kernel(
    groups, bands, chunk, block, tile, table,
    x_ref, matrix_ref, merid_ref, scale_ref, scale_out_ref, out_ref,
    got1, send2, got2, halo_out, halo_in, spectrum, send3, got3, send4, got4, matrix,
    load_sem, send_sem, recv_sem, halo_send, halo_recv,
):
    band = lax.axis_index("lat")
    me = lax.axis_index("lon")
    pair, core = me // 2, me % 2
    padded = groups * chunk
    half = block // 2
    mate = me + 1 - 2 * core
    across = band - 1 + 2 * core
    has_across = (across >= 0) & (across < bands)

    load = pltpu.make_async_copy(matrix_ref.at[pair], matrix, load_sem)
    load.start()
    barrier = pltpu.get_barrier_semaphore()
    for step in range(1, groups):
        pl.semaphore_signal(
            barrier, inc=1, device_id=(band, (me + step) % groups), device_id_type=MESH
        )

    @pl.when(has_across)
    def _():
        pl.semaphore_signal(barrier, inc=1, device_id=(across, mate), device_id_type=MESH)

    pl.semaphore_wait(barrier, groups - 1 + has_across.astype(jnp.int32))

    def rows(index):
        return pl.ds(pl.multiple_of(index * chunk, 8), chunk)

    def exchange(phase, source, target):
        def copies(step, to, slot):
            return [
                pltpu.make_async_remote_copy(
                    src_ref=piece,
                    dst_ref=place,
                    send_sem=send_sem.at[phase, step, part],
                    recv_sem=recv_sem.at[phase, step, part],
                    device_id=(band, to),
                    device_id_type=MESH,
                )
                for part, (piece, place) in enumerate(zip(source(to), target(slot)))
            ]

        started = []
        for step in range(1, groups):
            started.append(copies(step, (me + step) % groups, me))
            for copy in started[-1]:
                copy.start()

        def finish():
            for step in range(1, groups):
                origin = (me - step + groups) % groups
                for copy in copies(step, origin, origin):
                    copy.wait_recv()

        def drain():
            for batch in started:
                for copy in batch:
                    copy.wait_send()

        return finish, drain

    finish1, drain1 = exchange(0, lambda to: [x_ref.at[rows(to)]], lambda slot: [got1.at[slot]])
    got1[me] = x_ref[rows(me), :]
    finish1()
    for side in range(2):
        lanes = slice(side * block, (side + 1) * block)
        values = [got1[place, :, lanes] for place in range(groups)]
        for row in range(groups):
            send2[row // 2, side, row % 2] = weighted(values, table[row])
    finish2, drain2 = exchange(
        1,
        lambda to: [send2.at[to // 2, to % 2]],
        lambda slot: [got2.at[:, rows(slot), :]],
    )
    got2[:, rows(me), :] = send2[pair, core]
    load.wait()
    finish2()

    cells = parted(got2[...].reshape(2 * padded, block))

    def forward(index, carry):
        span = pl.ds(pl.multiple_of(index * tile, 128), tile)
        spectrum[span, :] = (
            product((matrix[0, span, :], matrix[1, span, :]), cells) * scale_ref[span, :]
        )
        return carry

    lax.fori_loop(0, 2 * padded // tile, forward, 0)

    upper, lower = spectrum[:padded, :], spectrum[padded:, :]
    left = lax.broadcasted_iota(jnp.int32, (padded, block), 1) < half
    halo_out[0] = jnp.where(left, pltpu.roll(upper, half, 1), lower)
    halo_out[1] = jnp.where(left, upper, pltpu.roll(lower, half, 1))

    def halo(slot, to_band):
        return pltpu.make_async_remote_copy(
            src_ref=halo_out.at[slot],
            dst_ref=halo_in.at[slot],
            send_sem=halo_send.at[slot],
            recv_sem=halo_recv.at[slot],
            device_id=(to_band, mate),
            device_id_type=MESH,
        )

    go_up = (core == 0) | (band < bands - 1)
    go_down = (core == 1) | (band > 0)
    up, down = halo(0, band + core), halo(1, band - 1 + core)

    @pl.when(go_up)
    def _():
        up.start()

    @pl.when(go_down)
    def _():
        down.start()

    @pl.when(jnp.logical_not(go_down))
    def _():
        halo_in[0] = jnp.zeros((padded, block), jnp.float32)

    @pl.when(jnp.logical_not(go_up))
    def _():
        halo_in[1] = jnp.zeros((padded, block), jnp.float32)

    own = product(parted(spectrum[...]), parted(merid_ref[:block, :]))

    @pl.when(go_down)
    def _():
        halo(0, band - 1 + core).wait_recv()

    @pl.when(go_up)
    def _():
        halo(1, band + core).wait_recv()

    below, above = halo_in[0], halo_in[1]
    beside = jnp.concatenate(
        [
            jnp.where(left, below, pltpu.roll(above, half, 1)),
            jnp.where(left, pltpu.roll(below, half, 1), above),
        ],
        axis=0,
    )
    mixed = own + product(parted(beside), parted(merid_ref[block:, :]))
    turned = parted((mixed * scale_out_ref[...]).T)

    def backward(index, carry):
        span = pl.ds(pl.multiple_of(index * tile, 128), tile)
        send3[span, :] = product(turned, (matrix[0, :, span], matrix[1, :, span])).T
        return carry

    lax.fori_loop(0, 2 * padded // tile, backward, 0)

    def portions(to):
        return [
            send3.at[pl.ds(pl.multiple_of(part * padded + to * chunk, 8), chunk)]
            for part in range(2)
        ]

    finish3, drain3 = exchange(2, portions, lambda slot: [got3.at[slot, 0], got3.at[slot, 1]])
    for part in range(2):
        got3[me, part] = send3[pl.ds(pl.multiple_of(part * padded + me * chunk, 8), chunk), :]
    finish3()
    for side in range(2):
        lanes = slice(side * block, (side + 1) * block)
        values = [got3[2 * (row // 2) + side, row % 2] for row in range(groups)]
        for place in range(groups):
            send4[place, :, lanes] = weighted(values, table[:, place])
    finish4, drain4 = exchange(3, lambda to: [send4.at[to]], lambda slot: [got4.at[rows(slot)]])
    got4[rows(me), :] = send4[me]
    finish4()
    out_ref[...] = got4[...]
    for drain in (drain1, drain2, drain3, drain4):
        drain()

    @pl.when(go_up)
    def _():
        up.wait_send()

    @pl.when(go_down)
    def _():
        down.wait_send()


def local(
    surface_forcing,
    ocean_mask,
    self_coupling,
    east_coupling,
    north_coupling,
    zonal_weight,
    aligned_inverse,
    staggered_inverse,
):
    groups, bands = lax.axis_size("lon"), lax.axis_size("lat")
    band, me = lax.axis_index("lat"), lax.axis_index("lon")
    length, columns = surface_forcing.shape
    block = aligned_inverse.shape[1]
    half = block // 2
    assert columns == 2 * block and groups % 2 == 0
    chunk = -(-length // (8 * groups)) * 8
    padded = groups * chunk
    while 2 * padded % 128:
        chunk, padded = chunk + 8, padded + 8 * groups
    width = 2 * padded
    tile = next(t for t in (384, 256, 128) if width % t == 0)
    table = outer_table(groups)
    matrix, waves, weights = inner_tables(groups, length, padded)
    pair, core = me // 2, me % 2

    wave = lax.dynamic_index_in_dim(jnp.asarray(waves), pair, 0, False)
    weight = lax.dynamic_index_in_dim(jnp.asarray(weights), pair, 0, False)
    zonal = lax.dynamic_slice_in_dim(zonal_weight, core * block, block)
    scale = lax.rsqrt(1.0 + wave[:, None] * zonal[None, :])
    scale_out = scale * weight[:, None]

    count = aligned_inverse.shape[0]
    carried = lax.ppermute(
        staggered_inverse[count - 1], "lat", [(i, i + 1) for i in range(bands - 1)]
    )
    aligned = lax.dynamic_index_in_dim(aligned_inverse, core, 0, False)
    above = lax.dynamic_index_in_dim(staggered_inverse, core, 0, False)
    below = jnp.where(core == 0, carried, staggered_inverse[0])
    zero = jnp.zeros((half, half), jnp.float32)
    inside = aligned + jnp.block([[below[half:, half:], zero], [zero, above[:half, :half]]])
    beside = jnp.block([[below[half:, :half], zero], [zero, above[:half, half:]]])
    merid = jnp.concatenate([inside, beside], axis=1).T

    f32 = jnp.float32
    vmem = pl.BlockSpec(memory_space=pltpu.VMEM)
    call = pl.pallas_call(
        functools.partial(kernel, groups, bands, chunk, block, tile, table),
        out_shape=jax.ShapeDtypeStruct((padded, columns), f32),
        in_specs=[vmem, pl.BlockSpec(memory_space=pl.ANY), vmem, vmem, vmem],
        out_specs=vmem,
        scratch_shapes=[
            pltpu.VMEM((groups, chunk, columns), f32),
            pltpu.VMEM((groups // 2, 2, 2, chunk, block), f32),
            pltpu.VMEM((2, padded, block), f32),
            pltpu.VMEM((2, padded, block), f32),
            pltpu.VMEM((2, padded, block), f32),
            pltpu.VMEM((width, block), f32),
            pltpu.VMEM((width, block), f32),
            pltpu.VMEM((groups, 2, chunk, block), f32),
            pltpu.VMEM((groups, chunk, columns), f32),
            pltpu.VMEM((padded, columns), f32),
            pltpu.VMEM((2, width, width), jnp.bfloat16),
            pltpu.SemaphoreType.DMA,
            pltpu.SemaphoreType.DMA((4, groups, 2)),
            pltpu.SemaphoreType.DMA((4, groups, 2)),
            pltpu.SemaphoreType.DMA((2,)),
            pltpu.SemaphoreType.DMA((2,)),
        ],
        compiler_params=pltpu.CompilerParams(
            collective_id=0, has_side_effects=True, vmem_limit_bytes=40 * 2**20
        ),
        cost_estimate=pl.CostEstimate(
            flops=40_000 * width * block, bytes_accessed=8 * width * width, transcendentals=0
        ),
        name="zonal_precondition",
    )
    constants = jnp.asarray(matrix)

    def precondition(field):
        grown = jnp.pad(field, ((0, padded - length), (0, 0)))
        return call(grown, constants, merid, scale, scale_out)[:length]

    ring = [(i, (i + 1) % groups) for i in range(groups)]
    back_ring = [(b, a) for a, b in ring]
    line = [(i, i + 1) for i in range(bands - 1)]
    back_line = [(b, a) for a, b in line]

    wet = ocean_mask.astype(f32)
    east_wet = east_coupling * wet
    north_wet = north_coupling * wet
    wet_east = jnp.concatenate([wet[1:], lax.ppermute(wet[:1], "lon", back_ring)], axis=0)
    wet_north = jnp.concatenate([wet[:, 1:], lax.ppermute(wet[:, :1], "lat", back_line)], axis=1)
    east_west = jnp.concatenate([lax.ppermute(east_wet[-1:], "lon", ring), east_wet[:-1]], axis=0)
    north_south = jnp.concatenate(
        [lax.ppermute(north_wet[:, -1:], "lat", line), north_wet[:, :-1]], axis=1
    )
    east = east_wet * wet_east
    north = north_wet * wet_north
    west = east_west * wet
    south = north_south * wet

    rhs_wet = wet * surface_forcing
    first = wet * precondition(rhs_wet)
    from_east = lax.ppermute(first[:1], "lon", back_ring)
    from_west = lax.ppermute(first[-1:], "lon", ring)
    from_north = lax.ppermute(first[:, :1], "lat", back_line)
    from_south = lax.ppermute(first[:, -1:], "lat", line)
    image = (1.0 - wet) * first + wet * self_coupling * first
    image = image + east * (first - jnp.concatenate([first[1:], from_east], axis=0))
    image = image + west * (first - jnp.concatenate([from_west, first[:-1]], axis=0))
    image = image + north * (first - jnp.concatenate([first[:, 1:], from_north], axis=1))
    image = image + south * (first - jnp.concatenate([from_south, first[:, :-1]], axis=1))
    sums = lax.psum(
        jnp.stack([jnp.sum(rhs_wet * first), jnp.sum(first * image)]), ("lat", "lon")
    )
    rz_now = sums[0]
    alpha = rz_now / sums[1]
    filtered = wet * precondition(image)
    solved = alpha * first
    residual = rhs_wet - alpha * image
    second = first - alpha * filtered
    rz_next = lax.psum(jnp.sum(residual * second), ("lat", "lon"))
    direction = second + rz_next / rz_now * first
    return (solved, residual, direction)


def solution(mesh):
    grid = P("lon", "lat")
    stack = P("lat", None, None)
    return jax.shard_map(
        local,
        mesh=mesh,
        in_specs=(grid, grid, grid, grid, grid, P("lat"), stack, stack),
        out_specs=(grid, grid, grid),
        check_vma=False,
    )
```

```python
import functools

import jax
import jax.numpy as jnp
import numpy as np
from jax import lax
from jax.experimental import pallas as pl
from jax.experimental.pallas import tpu as pltpu
from jax.sharding import PartitionSpec as P

MESH = pl.DeviceIdType.MESH


def outer_table(groups):
    table = np.zeros((groups, groups))
    place = np.arange(groups)
    table[0] = 1.0
    table[1] = np.where(place % 2 == 0, 1.0, -1.0)
    for mode in range(1, groups // 2):
        turn = 2.0 * np.pi * (mode * place % groups) / groups
        table[2 * mode] = np.cos(turn)
        table[2 * mode + 1] = -np.sin(turn)
    table[np.abs(table) < 1e-12] = 0.0
    return table


def inner_tables(groups, length, padded):
    total = groups * length
    pairs = groups // 2
    matrix = np.zeros((pairs, 2 * padded, 2 * padded))
    waves = np.zeros((pairs, 2 * padded))
    weights = np.zeros((pairs, 2 * padded))
    cell = np.arange(length)

    def turns(modes):
        return 2.0 * np.pi * (modes[:, None] * cell[None, :] % total) / total

    def note(pair, start, modes):
        stop = start + len(modes)
        waves[pair, start:stop] = 2.0 - 2.0 * np.cos(2.0 * np.pi * modes / total)
        weights[pair, start:stop] = np.where(modes * 2 % total == 0, 1.0, 2.0) / total

    for part, (first, real_count) in enumerate(((0, length // 2 + 1), (groups // 2, (length + 1) // 2))):
        skipped = 1 if part == 0 else 0
        real = first + groups * np.arange(real_count)
        imag = first + groups * (skipped + np.arange(length - real_count))
        row = part * padded
        columns = slice(part * padded, part * padded + length)
        matrix[0, row : row + real_count, columns] = np.cos(turns(real))
        matrix[0, row + real_count : row + length, columns] = -np.sin(turns(imag))
        note(0, row, real)
        note(0, row + real_count, imag)
    for pair in range(1, pairs):
        modes = pair + groups * np.arange(length)
        angle = turns(modes)
        low, high = slice(0, length), slice(padded, padded + length)
        matrix[pair, low, low] = np.cos(angle)
        matrix[pair, low, high] = np.sin(angle)
        matrix[pair, high, low] = -np.sin(angle)
        matrix[pair, high, high] = np.cos(angle)
        note(pair, 0, modes)
        note(pair, padded, modes)
    single = matrix.astype(np.float32)
    leading = single.astype(jnp.bfloat16)
    rest = (matrix - leading.astype(np.float64)).astype(jnp.bfloat16)
    return np.stack([leading, rest], axis=1), waves.astype(np.float32), weights.astype(np.float32)


def parted(value):
    leading = value.astype(jnp.bfloat16)
    return leading, (value - leading.astype(jnp.float32)).astype(jnp.bfloat16)


def product(left, right):
    dot = functools.partial(jnp.dot, preferred_element_type=jnp.float32)
    return dot(left[0], right[0]) + (dot(left[0], right[1]) + dot(left[1], right[0]))


def weighted(values, factors):
    total = None
    for value, factor in zip(values, factors):
        if factor == 0.0:
            continue
        term = value if factor == 1.0 else value * np.float32(factor)
        total = term if total is None else total + term
    return total


def kernel(
    groups, bands, chunk, block, tile, table,
    x_ref, matrix_ref, merid_ref, scale_ref, scale_out_ref, out_ref,
    got1, send2, got2, halo_out, halo_in, spectrum, send3, got3, send4, got4, matrix,
    load_sem, send_sem, recv_sem, halo_send, halo_recv,
):
    band = lax.axis_index("lat")
    me = lax.axis_index("lon")
    pair, core = me // 2, me % 2
    padded = groups * chunk
    half = block // 2
    mate = me + 1 - 2 * core
    across = band - 1 + 2 * core
    has_across = (across >= 0) & (across < bands)

    load = pltpu.make_async_copy(matrix_ref.at[pair], matrix, load_sem)
    load.start()
    barrier = pltpu.get_barrier_semaphore()
    for step in range(1, groups):
        pl.semaphore_signal(
            barrier, inc=1, device_id=(band, (me + step) % groups), device_id_type=MESH
        )

    @pl.when(has_across)
    def _():
        pl.semaphore_signal(barrier, inc=1, device_id=(across, mate), device_id_type=MESH)

    pl.semaphore_wait(barrier, groups - 1 + has_across.astype(jnp.int32))

    def rows(index):
        return pl.ds(pl.multiple_of(index * chunk, 8), chunk)

    def exchange(phase, source, target):
        def copies(step, to, slot):
            return [
                pltpu.make_async_remote_copy(
                    src_ref=piece,
                    dst_ref=place,
                    send_sem=send_sem.at[phase, step, part],
                    recv_sem=recv_sem.at[phase, step, part],
                    device_id=(band, to),
                    device_id_type=MESH,
                )
                for part, (piece, place) in enumerate(zip(source(to), target(slot)))
            ]

        started = []
        for step in range(1, groups):
            started.append(copies(step, (me + step) % groups, me))
            for copy in started[-1]:
                copy.start()

        def finish():
            for step in range(1, groups):
                origin = (me - step + groups) % groups
                for copy in copies(step, origin, origin):
                    copy.wait_recv()

        def drain():
            for batch in started:
                for copy in batch:
                    copy.wait_send()

        return finish, drain

    finish1, drain1 = exchange(0, lambda to: [x_ref.at[rows(to)]], lambda slot: [got1.at[slot]])
    got1[me] = x_ref[rows(me), :]
    finish1()
    for side in range(2):
        lanes = slice(side * block, (side + 1) * block)
        values = [got1[place, :, lanes] for place in range(groups)]
        for row in range(groups):
            send2[row // 2, side, row % 2] = weighted(values, table[row])
    finish2, drain2 = exchange(
        1,
        lambda to: [send2.at[to // 2, to % 2]],
        lambda slot: [got2.at[:, rows(slot), :]],
    )
    got2[:, rows(me), :] = send2[pair, core]
    load.wait()
    finish2()

    cells = parted(got2[...].reshape(2 * padded, block))

    def forward(index, carry):
        span = pl.ds(pl.multiple_of(index * tile, 128), tile)
        spectrum[span, :] = (
            product((matrix[0, span, :], matrix[1, span, :]), cells) * scale_ref[span, :]
        )
        return carry

    lax.fori_loop(0, 2 * padded // tile, forward, 0)

    upper, lower = spectrum[:padded, :], spectrum[padded:, :]
    left = lax.broadcasted_iota(jnp.int32, (padded, block), 1) < half
    halo_out[0] = jnp.where(left, pltpu.roll(upper, half, 1), lower)
    halo_out[1] = jnp.where(left, upper, pltpu.roll(lower, half, 1))

    def halo(slot, to_band):
        return pltpu.make_async_remote_copy(
            src_ref=halo_out.at[slot],
            dst_ref=halo_in.at[slot],
            send_sem=halo_send.at[slot],
            recv_sem=halo_recv.at[slot],
            device_id=(to_band, mate),
            device_id_type=MESH,
        )

    go_up = (core == 0) | (band < bands - 1)
    go_down = (core == 1) | (band > 0)
    up, down = halo(0, band + core), halo(1, band - 1 + core)

    @pl.when(go_up)
    def _():
        up.start()

    @pl.when(go_down)
    def _():
        down.start()

    @pl.when(jnp.logical_not(go_down))
    def _():
        halo_in[0] = jnp.zeros((padded, block), jnp.float32)

    @pl.when(jnp.logical_not(go_up))
    def _():
        halo_in[1] = jnp.zeros((padded, block), jnp.float32)

    own = product(parted(spectrum[...]), parted(merid_ref[:block, :]))

    @pl.when(go_down)
    def _():
        halo(0, band - 1 + core).wait_recv()

    @pl.when(go_up)
    def _():
        halo(1, band + core).wait_recv()

    below, above = halo_in[0], halo_in[1]
    beside = jnp.concatenate(
        [
            jnp.where(left, below, pltpu.roll(above, half, 1)),
            jnp.where(left, pltpu.roll(below, half, 1), above),
        ],
        axis=0,
    )
    mixed = own + product(parted(beside), parted(merid_ref[block:, :]))
    turned = parted((mixed * scale_out_ref[...]).T)

    def backward(index, carry):
        span = pl.ds(pl.multiple_of(index * tile, 128), tile)
        send3[span, :] = product(turned, (matrix[0, :, span], matrix[1, :, span])).T
        return carry

    lax.fori_loop(0, 2 * padded // tile, backward, 0)

    def portions(to):
        return [
            send3.at[pl.ds(pl.multiple_of(part * padded + to * chunk, 8), chunk)]
            for part in range(2)
        ]

    finish3, drain3 = exchange(2, portions, lambda slot: [got3.at[slot, 0], got3.at[slot, 1]])
    for part in range(2):
        got3[me, part] = send3[pl.ds(pl.multiple_of(part * padded + me * chunk, 8), chunk), :]
    finish3()
    for side in range(2):
        lanes = slice(side * block, (side + 1) * block)
        values = [got3[2 * (row // 2) + side, row % 2] for row in range(groups)]
        for place in range(groups):
            send4[place, :, lanes] = weighted(values, table[:, place])
    finish4, drain4 = exchange(3, lambda to: [send4.at[to]], lambda slot: [got4.at[rows(slot)]])
    got4[rows(me), :] = send4[me]
    finish4()
    out_ref[...] = got4[...]
    for drain in (drain1, drain2, drain3, drain4):
        drain()

    @pl.when(go_up)
    def _():
        up.wait_send()

    @pl.when(go_down)
    def _():
        down.wait_send()


def total_kernel(groups, bands, x_ref, out_ref, circle, middle, column, send_sem, recv_sem):
    band = lax.axis_index("lat")
    me = lax.axis_index("lon")
    barrier = pltpu.get_barrier_semaphore()
    for step in range(1, groups):
        pl.semaphore_signal(
            barrier, inc=1, device_id=(band, (me + step) % groups), device_id_type=MESH
        )
    for step in range(1, bands):
        pl.semaphore_signal(
            barrier, inc=1, device_id=((band + step) % bands, me), device_id_type=MESH
        )
    pl.semaphore_wait(barrier, groups + bands - 2)

    def gather(source, target, place, count, first, address):
        def copy(step, to, slot):
            return pltpu.make_async_remote_copy(
                src_ref=source,
                dst_ref=target.at[slot],
                send_sem=send_sem.at[first + step],
                recv_sem=recv_sem.at[first + step],
                device_id=address(to),
                device_id_type=MESH,
            )

        sent = [copy(step, (place + step) % count, place) for step in range(1, count)]
        for item in sent:
            item.start()
        target[place] = source[...]
        for step in range(1, count):
            origin = (place - step + count) % count
            copy(step, origin, origin).wait_recv()
        total = target[0]
        for index in range(1, count):
            total = total + target[index]
        return total, sent

    total, sent1 = gather(x_ref, circle, me, groups, 0, lambda to: (band, to))
    middle[...] = total
    total, sent2 = gather(middle, column, band, bands, groups, lambda to: (to, me))
    out_ref[...] = total
    for item in sent1 + sent2:
        item.wait_send()


def totals(values):
    groups, bands = lax.axis_size("lon"), lax.axis_size("lat")
    tile = jnp.zeros((8, 128), jnp.float32)
    row = lax.broadcasted_iota(jnp.int32, (8, 128), 0)
    for index, value in enumerate(values):
        tile = jnp.where(row == index, value, tile)
    vmem = pl.BlockSpec(memory_space=pltpu.VMEM)
    summed = pl.pallas_call(
        functools.partial(total_kernel, groups, bands),
        out_shape=jax.ShapeDtypeStruct((8, 128), jnp.float32),
        in_specs=[vmem],
        out_specs=vmem,
        scratch_shapes=[
            pltpu.VMEM((groups, 8, 128), jnp.float32),
            pltpu.VMEM((8, 128), jnp.float32),
            pltpu.VMEM((bands, 8, 128), jnp.float32),
            pltpu.SemaphoreType.DMA((groups + bands,)),
            pltpu.SemaphoreType.DMA((groups + bands,)),
        ],
        compiler_params=pltpu.CompilerParams(collective_id=1, has_side_effects=True),
        cost_estimate=pl.CostEstimate(flops=10_000_000, bytes_accessed=8192, transcendentals=0),
        name="total",
    )(tile)
    return [summed[index, 0] for index in range(len(values))]


def local(
    surface_forcing,
    ocean_mask,
    self_coupling,
    east_coupling,
    north_coupling,
    zonal_weight,
    aligned_inverse,
    staggered_inverse,
):
    groups, bands = lax.axis_size("lon"), lax.axis_size("lat")
    band, me = lax.axis_index("lat"), lax.axis_index("lon")
    length, columns = surface_forcing.shape
    block = aligned_inverse.shape[1]
    half = block // 2
    assert columns == 2 * block and groups % 2 == 0
    chunk = -(-length // (8 * groups)) * 8
    padded = groups * chunk
    while 2 * padded % 128:
        chunk, padded = chunk + 8, padded + 8 * groups
    width = 2 * padded
    tile = next(t for t in (384, 256, 128) if width % t == 0)
    table = outer_table(groups)
    matrix, waves, weights = inner_tables(groups, length, padded)
    pair, core = me // 2, me % 2

    wave = lax.dynamic_index_in_dim(jnp.asarray(waves), pair, 0, False)
    weight = lax.dynamic_index_in_dim(jnp.asarray(weights), pair, 0, False)
    zonal = lax.dynamic_slice_in_dim(zonal_weight, core * block, block)
    scale = lax.rsqrt(1.0 + wave[:, None] * zonal[None, :])
    scale_out = scale * weight[:, None]

    count = aligned_inverse.shape[0]
    carried = lax.ppermute(
        staggered_inverse[count - 1], "lat", [(i, i + 1) for i in range(bands - 1)]
    )
    aligned = lax.dynamic_index_in_dim(aligned_inverse, core, 0, False)
    above = lax.dynamic_index_in_dim(staggered_inverse, core, 0, False)
    below = jnp.where(core == 0, carried, staggered_inverse[0])
    zero = jnp.zeros((half, half), jnp.float32)
    inside = aligned + jnp.block([[below[half:, half:], zero], [zero, above[:half, :half]]])
    beside = jnp.block([[below[half:, :half], zero], [zero, above[:half, half:]]])
    merid = jnp.concatenate([inside, beside], axis=1).T

    f32 = jnp.float32
    vmem = pl.BlockSpec(memory_space=pltpu.VMEM)
    call = pl.pallas_call(
        functools.partial(kernel, groups, bands, chunk, block, tile, table),
        out_shape=jax.ShapeDtypeStruct((padded, columns), f32),
        in_specs=[vmem, pl.BlockSpec(memory_space=pl.ANY), vmem, vmem, vmem],
        out_specs=vmem,
        scratch_shapes=[
            pltpu.VMEM((groups, chunk, columns), f32),
            pltpu.VMEM((groups // 2, 2, 2, chunk, block), f32),
            pltpu.VMEM((2, padded, block), f32),
            pltpu.VMEM((2, padded, block), f32),
            pltpu.VMEM((2, padded, block), f32),
            pltpu.VMEM((width, block), f32),
            pltpu.VMEM((width, block), f32),
            pltpu.VMEM((groups, 2, chunk, block), f32),
            pltpu.VMEM((groups, chunk, columns), f32),
            pltpu.VMEM((padded, columns), f32),
            pltpu.VMEM((2, width, width), jnp.bfloat16),
            pltpu.SemaphoreType.DMA,
            pltpu.SemaphoreType.DMA((4, groups, 2)),
            pltpu.SemaphoreType.DMA((4, groups, 2)),
            pltpu.SemaphoreType.DMA((2,)),
            pltpu.SemaphoreType.DMA((2,)),
        ],
        compiler_params=pltpu.CompilerParams(
            collective_id=0, has_side_effects=True, vmem_limit_bytes=40 * 2**20
        ),
        cost_estimate=pl.CostEstimate(
            flops=40_000 * width * block, bytes_accessed=8 * width * width, transcendentals=0
        ),
        name="zonal_precondition",
    )
    constants = jnp.asarray(matrix)

    def precondition(field):
        grown = jnp.pad(field, ((0, padded - length), (0, 0)))
        return call(grown, constants, merid, scale, scale_out)[:length]

    ring = [(i, (i + 1) % groups) for i in range(groups)]
    back_ring = [(b, a) for a, b in ring]
    line = [(i, i + 1) for i in range(bands - 1)]
    back_line = [(b, a) for a, b in line]

    wet = ocean_mask.astype(f32)
    east_wet = east_coupling * wet
    north_wet = north_coupling * wet
    wet_east = jnp.concatenate([wet[1:], lax.ppermute(wet[:1], "lon", back_ring)], axis=0)
    wet_north = jnp.concatenate([wet[:, 1:], lax.ppermute(wet[:, :1], "lat", back_line)], axis=1)
    east_west = jnp.concatenate([lax.ppermute(east_wet[-1:], "lon", ring), east_wet[:-1]], axis=0)
    north_south = jnp.concatenate(
        [lax.ppermute(north_wet[:, -1:], "lat", line), north_wet[:, :-1]], axis=1
    )
    east = east_wet * wet_east
    north = north_wet * wet_north
    west = east_west * wet
    south = north_south * wet

    rhs_wet = wet * surface_forcing
    first = wet * precondition(rhs_wet)
    from_east = lax.ppermute(first[:1], "lon", back_ring)
    from_west = lax.ppermute(first[-1:], "lon", ring)
    from_north = lax.ppermute(first[:, :1], "lat", back_line)
    from_south = lax.ppermute(first[:, -1:], "lat", line)
    image = (1.0 - wet) * first + wet * self_coupling * first
    image = image + east * (first - jnp.concatenate([first[1:], from_east], axis=0))
    image = image + west * (first - jnp.concatenate([from_west, first[:-1]], axis=0))
    image = image + north * (first - jnp.concatenate([first[:, 1:], from_north], axis=1))
    image = image + south * (first - jnp.concatenate([from_south, first[:, :-1]], axis=1))
    rz_now, curvature = totals([jnp.sum(rhs_wet * first), jnp.sum(first * image)])
    alpha = rz_now / curvature
    filtered = wet * precondition(image)
    solved = alpha * first
    residual = rhs_wet - alpha * image
    second = first - alpha * filtered
    (rz_next,) = totals([jnp.sum(residual * second)])
    direction = second + rz_next / rz_now * first
    return (solved, residual, direction)


def solution(mesh):
    grid = P("lon", "lat")
    stack = P("lat", None, None)
    return jax.shard_map(
        local,
        mesh=mesh,
        in_specs=(grid, grid, grid, grid, grid, P("lat"), stack, stack),
        out_specs=(grid, grid, grid),
        check_vma=False,
    )
```
